32 devices in a mesh: dp: 4 (over y, x), expert: 8 (over z, core).
Axes of the slice: x: 2, y: 2, z: 4, core: 2. Of those that a mesh axis runs over, the one named last changes fastest.
Arguments:
- inputs: bfloat16 [16384, 768], P(('dp', 'expert')), may hold values from -6 to 6
- cotangent: bfloat16 [16384, 768], P(('dp', 'expert')), may hold values from -6 to 6
- lengths: int32 [32], P(('dp', 'expert')), may hold values from 384 to 512, as said below
- routes: int32 [16384, 2], P(('dp', 'expert')), may hold values from 0 to 7, all different within a row; in each aligned block of 512 rows (0 to 511, 512 to 1023, ...) at most 192 rows name the same one
- w_qkv: bfloat16 [768, 2304], P('dp'), may hold values from -0.21875 to 0.21875
- w_attn_out: bfloat16 [768, 768], P('dp'), may hold values from -1.25 to 1.25
- w_router: bfloat16 [768, 8], P('dp'), may hold values from -0.4375 to 0.4375
- gain_attn: bfloat16 [768], P('dp'), may hold values from 0.5 to 1.5
- gain_moe: bfloat16 [768], P('dp'), may hold values from 0.5 to 1.5
- rel_bias: bfloat16 [12, 32], P('dp'), may hold values from -4 to 4
- w_in: bfloat16 [8, 768, 3072], P('expert'), may hold values from -0.21875 to 0.21875
- w_out: bfloat16 [8, 768, 3072], P('expert'), may hold values from -0.109375 to 0.109375
Outputs:
- outputs: bfloat16 [16384, 768], P(('dp', 'expert'))
- d_inputs: bfloat16 [16384, 768], P(('dp', 'expert'))
- grad_qkv: float32 [768, 2304], P('dp')
- grad_attn_out: float32 [768, 768], P('dp')
- grad_router: float32 [768, 8], P('dp')
- grad_gain_attn: float32 [768], P('dp')
- grad_gain_moe: float32 [768], P('dp')
- grad_rel_bias: float32 [12, 32], P('dp')
- grad_w_in: float32 [8, 768, 3072], P('expert', None, 'dp')
- grad_w_out: float32 [8, 768, 3072], P('expert', None, 'dp')
The draws below stay inside these ranges and needn't reach their ends.
Inputs may be any that keep to these rules, and one draw needn't show every extreme that they name: `lengths`: slots of a sequence at or past its length are padding; some sequence is full and some has the fewest valid tokens. `routes`: a token names two different experts; in the rows of one device no expert is named more than 192 times, a bound that some block reaches.
All inputs are finite; a program needn't handle non-finite values.
Results may differ from the reference program's by a relative error of at most 0.018.
Values may be sent and summed in bfloat16 or wider, within the bound.
A program may use at most 256 MiB of HBM per device.

```python
import math
import jax
import jax.numpy as jnp
import numpy as np
from jax import lax

D = 768
HEADS = 12
HDIM = 64
FF = 3072
TOP = 2
BUCKETS = 32
TOK_DEV = 512
NSEQ = 32
TOKENS = 16384
EXPERTS = 8
CAP = 192


def draw_lengths(key, part):
    key_base, key_perm = jax.random.split(key)
    lowest_len = 3 * TOK_DEV // 4
    drawn_len = jax.random.randint(key_base, (NSEQ,), lowest_len, TOK_DEV + 1)
    shuffled = jax.random.permutation(key_perm, NSEQ)
    position = jnp.arange(NSEQ)
    drawn_len = jnp.where(position == shuffled[0], TOK_DEV, drawn_len)
    drawn_len = jnp.where(position == shuffled[1], lowest_len, drawn_len)
    return drawn_len.astype(jnp.int32)


def block_scale(stream_key, shape, pieces, smallest, high):
    gain, own = 1.0, jax.random.fold_in(stream_key, 6)
    for dim, shards_of in pieces:
        draws = jnp.exp(jax.random.uniform(jax.random.fold_in(own, dim), (shards_of,), jnp.float32, smallest / len(pieces), high / len(pieces)))
        gain = gain * jnp.repeat(draws, shape[dim] // shards_of).reshape([-1 if axis == dim else 1 for axis in range(len(shape))])
    return gain


def shared_out(own_key, own, number, rows, count, top, limit, slope):
    ranking = jax.random.permutation(own_key, count)
    heavy_load, ordinary = load_shares(count, rows * top, limit, slope, True), load_shares(count, rows * top, limit, slope, False)
    places = jnp.arange(count)

    def named(sizes, rotation):
        used = int((sizes > 0).sum())
        fixed = max(1, used // 4)
        moved = fixed + (places - fixed + rotation * (used - fixed)) % max(1, count - fixed)
        return jnp.zeros((count,), jnp.int32).at[ranking[jnp.where(places < fixed, places, moved)]].set(jnp.asarray(sizes, jnp.int32))

    sizes = jnp.where(number % 4 == 0, named(heavy_load, number // 4), named(ordinary, number - number // 4 - 1))
    mixed = jax.random.permutation(jax.random.fold_in(own, 3), count)
    giver, sink = mixed[0:count // 2 * 2:2], mixed[1:count // 2 * 2:2]
    room = jnp.minimum(sizes[giver] - 1, limit - sizes[sink]) // 2
    room = jnp.where((giver == ranking[0]) | (sink == ranking[0]) | (sizes[sink] == 0), 0, jnp.maximum(room, 0))
    moved = jax.random.randint(jax.random.fold_in(own, 4), (count // 2,), 0, 1 << 20) % (room + 1)
    sizes = sizes.at[giver].add(-moved).at[sink].add(moved)
    labels = jnp.searchsorted(jnp.cumsum(sizes), jnp.arange(rows * top), side="right").astype(jnp.int32)
    table = labels.reshape(top, rows).T
    table = table[jax.random.permutation(jax.random.fold_in(own, 1), rows)]
    rotation = jax.random.randint(jax.random.fold_in(own, 2), (rows, 1), 0, top)
    return jnp.take_along_axis(table, (jnp.arange(top)[None, :] + rotation) % top, axis=1)


def load_shares(count, total, limit, skew, full):
    weights = [(1 << 20) // math.isqrt(standing ** skew) + 1 for standing in range(1, count + 1)]
    largest = limit if full else min(limit, max(-(-total // count), total * weights[0] // sum(weights)))
    least = 1 if total - largest >= count - 1 else 0
    counts, surplus = [largest] + [least] * (count - 1), total - largest - least * (count - 1)
    while surplus > 0:
        free = [i for i in range(1, count) if counts[i] < largest] or [i for i in range(1, count) if counts[i] < limit]
        pool, remaining = sum([weights[i] for i in free]), surplus
        for i in free:
            more = min(limit - counts[i], max(1, remaining * weights[i] // pool), surplus)
            counts[i] = counts[i] + more
            surplus = surplus - more
    return np.array(counts)


def scatter_about(key, extent, deviation, limit, cuts=(), kind=jnp.bfloat16):
    loudness = block_scale(key, extent, cuts, -0.22, 0.18) if cuts else 1.0
    array = jax.random.normal(key, extent, jnp.float32) * deviation * loudness
    return jnp.minimum(jnp.maximum(array, -limit), limit).astype(kind)


def setup_inputs(seed: int = 0) -> dict:
    arg_keys = jax.random.split(jax.random.key(seed), 13)
    inputs = scatter_about(arg_keys[0], (TOKENS, D), 1.0, 6.0, ((0, 32),))
    cotangent = scatter_about(arg_keys[1], (TOKENS, D), 1.0, 6.0, ((0, 32),))
    lengths = draw_lengths(jax.random.fold_in(arg_keys[12], 71), 0)
    routes_keys = jax.random.split(jax.random.fold_in(arg_keys[3], 1), TOKENS // TOK_DEV)
    routes_turns = jax.random.permutation(jax.random.fold_in(arg_keys[3], 3), TOKENS // TOK_DEV)
    routes = jax.vmap(lambda own, number: shared_out(jax.random.fold_in(arg_keys[3], 2), own, number, TOK_DEV, EXPERTS, TOP, CAP, 1))(routes_keys, routes_turns).reshape((TOKENS, TOP))
    w_qkv = scatter_about(arg_keys[4], (D, 3 * D), D ** -0.5, 0.21875, ((0, 4),))
    w_attn_out = scatter_about(arg_keys[5], (D, D), (D // 32) ** -0.5, 1.25, ((0, 4),))
    w_router = scatter_about(arg_keys[6], (D, EXPERTS), (D // 4) ** -0.5, 0.4375, ((0, 4),))
    gain_attn = jnp.clip(1.0 + 0.1 * jax.random.normal(arg_keys[7], (D,), jnp.float32), 0.5, 1.5).astype(jnp.bfloat16)
    gain_moe = jnp.clip(1.0 + 0.1 * jax.random.normal(arg_keys[8], (D,), jnp.float32), 0.5, 1.5).astype(jnp.bfloat16)
    rel_bias = scatter_about(arg_keys[9], (HEADS, BUCKETS), 1.0, 4.0, ((0, 4),))
    w_in = scatter_about(arg_keys[10], (EXPERTS, D, FF), D ** -0.5, 0.21875, ((0, 8),))
    w_out = scatter_about(arg_keys[11], (EXPERTS, D, FF), FF ** -0.5, 0.109375, ((0, 8),))
    return {"inputs": inputs, "cotangent": cotangent, "lengths": lengths, "routes": routes, "w_qkv": w_qkv, "w_attn_out": w_attn_out, "w_router": w_router, "gain_attn": gain_attn, "gain_moe": gain_moe, "rel_bias": rel_bias, "w_in": w_in, "w_out": w_out}


norm_eps = 1e-06
rel_edges = (19, 21, 24, 27, 31, 35, 40, 46, 52, 59, 67, 77, 87, 99, 113)

@jax.custom_vjp
def low(v):
    return lax.optimization_barrier(v.astype(jnp.bfloat16)).astype(jnp.float32)

@jax.custom_vjp
def low_back(v):
    return v

def low_keep(v):
    return (low(v), None)

def low_pass(kept, grad):
    return (grad,)

def back_keep(v):
    return (v, None)

def back_low(kept, grad):
    return (low(grad),)
low.defvjp(low_keep, low_pass)
low_back.defvjp(back_keep, back_low)

def rms_apply(vector, gain_vec):
    return vector * lax.rsqrt(lax.optimization_barrier(jnp.mean(vector * vector, axis=-1, keepdims=True)) + norm_eps) * gain_vec

def bucket_of(distance):
    far_bucket = jnp.full(distance.shape, 16, jnp.int32)
    for edge_value in rel_edges:
        far_bucket = far_bucket + (distance >= edge_value).astype(jnp.int32)
    return jnp.where(distance < 16, distance, far_bucket).astype(jnp.int32)

def reference(inputs, cotangent, lengths, routes, w_qkv, w_attn_out, w_router, gain_attn, gain_moe, rel_bias, w_in, w_out):
    precise = lax.Precision.HIGHEST
    score_scale = HDIM ** (-0.5)
    positions = jnp.arange(TOK_DEV, dtype=jnp.int32)
    distance = positions[:, None] - positions[None, :]
    causal = distance >= 0
    bucket_map = bucket_of(jnp.maximum(distance, 0))
    valid_mask = positions[None, :] < lengths[:, None]
    valid_flat = valid_mask.astype(jnp.float32).reshape(TOKENS)
    flat_routes = routes.reshape(NSEQ, TOK_DEV * TOP)
    flat_valid = jnp.repeat(valid_mask, TOP, axis=1)
    route_hot = ((flat_routes[:, :, None] == jnp.arange(EXPERTS, dtype=jnp.int32)) & flat_valid[:, :, None]).astype(jnp.int32)
    rank_in = lax.optimization_barrier(jnp.sum((jnp.cumsum(route_hot, axis=1) - route_hot) * route_hot, axis=2))
    seq_ids = jnp.arange(NSEQ, dtype=jnp.int32)[:, None]
    spread = NSEQ * CAP
    slot_index = jnp.where(flat_valid, flat_routes * spread + seq_ids * CAP + rank_in, EXPERTS * spread).astype(jnp.int32)
    token_of_route = seq_ids * TOK_DEV + jnp.arange(TOK_DEV * TOP, dtype=jnp.int32)[None, :] // TOP
    source = jnp.zeros((EXPERTS * spread + 1,), jnp.int32).at[slot_index.reshape(-1)].set(token_of_route.reshape(-1).astype(jnp.int32))
    source = source[:-1].reshape(EXPERTS, spread)
    filled = jnp.zeros((EXPERTS * spread + 1,), jnp.float32).at[slot_index.reshape(-1)].set(1.0)
    filled = filled[:-1].reshape(EXPERTS, spread)
    slot_routes = slot_index.reshape(TOKENS, TOP)

    def block_forward(inputs_wide, proj_w, mix_w, gate_w, gain_first, gain_second, bias_table, first_w, second_w):

        def attend(packed):
            seq_rows, seq_keep = packed
            normed_attn = low(rms_apply(seq_rows, gain_first))
            proj_qkv = low(low_back(jnp.dot(normed_attn, proj_w, precision=precise)))
            query_heads = proj_qkv[:, :D].reshape(TOK_DEV, HEADS, HDIM)
            key_heads = proj_qkv[:, D:2 * D].reshape(TOK_DEV, HEADS, HDIM)
            value_heads = proj_qkv[:, 2 * D:].reshape(TOK_DEV, HEADS, HDIM)
            scores = jnp.einsum('qhd,khd->hqk', query_heads, key_heads, precision=precise) * score_scale + bias_table[:, bucket_map]
            allowed = causal & seq_keep[None, :]
            scores = low_back(jnp.where(allowed[None], scores, -1e+30))
            attn_prob = low(jax.nn.softmax(scores, axis=-1))
            attn_heads = jnp.einsum('hqk,khd->qhd', attn_prob, value_heads, precision=precise).reshape(TOK_DEV, D)
            attn_heads = low(low_back(attn_heads))
            attn_proj = low_back(jnp.dot(attn_heads, mix_w, precision=precise))
            return seq_rows + seq_keep.astype(jnp.float32)[:, None] * attn_proj
        hidden = lax.map(jax.checkpoint(attend), (inputs_wide.reshape(NSEQ, TOK_DEV, D), valid_mask)).reshape(TOKENS, D)
        normed_moe = low(rms_apply(hidden, gain_second))
        logits = low_back(jnp.dot(normed_moe, gate_w, precision=precise))
        chosen = jnp.take_along_axis(logits, routes, axis=1)
        gates = jax.nn.softmax(chosen, axis=-1) * valid_flat[:, None]

        def expert(packed):
            row_ids, row_fill, first_mat, second_mat = packed
            slot_rows = low_back(normed_moe[row_ids] * row_fill[:, None])
            pre_act = low_back(jnp.dot(slot_rows, first_mat, precision=precise))
            activation = low(jax.nn.gelu(pre_act))
            return low(low_back(jnp.dot(activation, second_mat.T, precision=precise)))
        expert_out = lax.map(jax.checkpoint(expert), (source, filled, first_w, second_w))
        out_table = jnp.concatenate([expert_out.reshape(EXPERTS * spread, D), jnp.zeros((1, D), jnp.float32)], axis=0)
        picked = out_table[slot_routes]
        moe_out = lax.optimization_barrier(jnp.sum(gates[:, :, None] * picked, axis=1))
        return valid_flat[:, None] * (hidden + moe_out)
    primals = (inputs.astype(jnp.float32), w_qkv.astype(jnp.float32), w_attn_out.astype(jnp.float32), w_router.astype(jnp.float32), gain_attn.astype(jnp.float32), gain_moe.astype(jnp.float32), rel_bias.astype(jnp.float32), w_in.astype(jnp.float32), w_out.astype(jnp.float32))
    result, pullback = jax.vjp(block_forward, *primals)
    gradients = pullback(cotangent.astype(jnp.float32))
    return (result.astype(jnp.bfloat16), gradients[0].astype(jnp.bfloat16), gradients[1], gradients[2], gradients[3], gradients[4], gradients[5], gradients[6], gradients[7], gradients[8])
```

```python
import functools
import math

import jax
import jax.numpy as jnp
from jax import lax
from jax.experimental import pallas as pl
from jax.experimental.pallas import tpu as pltpu
from jax.sharding import PartitionSpec as P

norm_eps = 1e-06
rel_edges = (19, 21, 24, 27, 31, 35, 40, 46, 52, 59, 67, 77, 87, 99, 113)
far_start = 113
bf16 = jnp.bfloat16
f32 = jnp.float32
neg_big = -1e30
tile = 128
gelu_c = math.sqrt(2.0 / math.pi)
gelu_k = 0.044715


def bucket_of(distance):
    far_bucket = jnp.full(distance.shape, 16, jnp.int32)
    for edge_value in rel_edges:
        far_bucket = far_bucket + (distance >= edge_value).astype(jnp.int32)
    return jnp.where(distance < 16, distance, far_bucket)


def mm(a, b, ca=1, cb=0):
    return lax.dot_general(a, b, (((ca,), (cb,)), ((), ())), preferred_element_type=f32)


def round_up(a, b):
    return (a + b - 1) // b * b


def head_tiles(rev_ref, hh):
    row = rev_ref[0, hh : hh + 1, :]
    toe = pltpu.roll(jnp.broadcast_to(row, (tile, 2 * tile)), 0, 1, stride=1, stride_axis=0)
    down = lax.broadcasted_iota(jnp.int32, (tile, tile), 0)
    across = lax.broadcasted_iota(jnp.int32, (tile, tile), 1)
    diag = jnp.where(down >= across, toe[:, :tile], neg_big)
    return diag, toe[:, tile:], jnp.broadcast_to(row[:, tile : tile + 1], (tile, tile))


def score_tiles(q_part, k_ref, km_ref, bias, qb, count):
    keys = (qb + 1) * tile
    raw = mm(q_part, k_ref[0:keys, :], 1, 1)
    out = []
    for kb in range(qb + 1):
        part = raw[:, kb * tile : (kb + 1) * tile] + bias[min(qb - kb, 2)]
        if (kb + 1) * tile > 3 * count // 4:
            part = part + km_ref[0:1, kb * tile : (kb + 1) * tile]
        out.append(part)
    return out


def attn_fwd_kernel(q_ref, k_ref, v_ref, rev_ref, km_ref, o_ref, lse_ref):
    count = q_ref.shape[0]
    width = q_ref.shape[1]
    lane = lax.broadcasted_iota(jnp.int32, (1, width), 1)
    first = lane < width // 2
    scale = jnp.asarray((width // 2) ** (-0.5), bf16)
    biases = [head_tiles(rev_ref, hh) for hh in range(2)]
    for qb in range(count // tile):
        rows = slice(qb * tile, (qb + 1) * tile)
        outs, lses = [], []
        for hh in range(2):
            mine = first if hh == 0 else jnp.logical_not(first)
            q_part = jnp.where(mine, q_ref[rows, :] * scale, jnp.zeros((), bf16))
            parts = score_tiles(q_part, k_ref, km_ref, biases[hh], qb, count)
            top = functools.reduce(jnp.maximum, parts)
            top = jnp.max(top, axis=1, keepdims=True)
            exps = [jnp.exp(part - top) for part in parts]
            total = jnp.sum(functools.reduce(jnp.add, exps), axis=1, keepdims=True)
            inv = 1.0 / total
            probs = jnp.concatenate([(e * inv).astype(bf16) for e in exps], axis=1)
            outs.append(mm(probs, v_ref[0 : (qb + 1) * tile, :]))
            lses.append(top + jnp.log(total))
        o_ref[rows, :] = jnp.where(first, outs[0], outs[1]).astype(bf16)
        lse_ref[0, rows, :] = jnp.where(first, lses[0], lses[1])


def attention_forward(qkv, rev, key_mask):
    count, three = qkv.shape
    width = three // 3
    pairs = width // tile
    return pl.pallas_call(
        attn_fwd_kernel,
        grid=(pairs,),
        in_specs=[
            pl.BlockSpec((count, tile), lambda h: (0, h)),
            pl.BlockSpec((count, tile), lambda h: (0, h + pairs)),
            pl.BlockSpec((count, tile), lambda h: (0, h + 2 * pairs)),
            pl.BlockSpec((1, 2, 2 * tile), lambda h: (h, 0, 0)),
            pl.BlockSpec((1, count), lambda h: (0, 0)),
        ],
        out_specs=[
            pl.BlockSpec((count, tile), lambda h: (0, h)),
            pl.BlockSpec((1, count, tile), lambda h: (h, 0, 0)),
        ],
        out_shape=[
            jax.ShapeDtypeStruct((count, width), bf16),
            jax.ShapeDtypeStruct((pairs, count, tile), f32),
        ],
        cost_estimate=pl.CostEstimate(
            flops=4 * count * count * width, bytes_accessed=16 * count * width, transcendentals=0
        ),
        name="attn_fwd",
    )(qkv, qkv, qkv, rev, key_mask)


def unskew(block):
    down = lax.broadcasted_iota(jnp.int32, block.shape, 0)
    lanes = block.shape[1]
    step = 1
    while step < block.shape[0]:
        moved = pltpu.roll(block, lanes - step, 1)
        block = jnp.where((down & step) != 0, moved, block)
        step *= 2
    return block


def attn_bwd_kernel(
    q_ref, k_ref, v_ref, do_ref, lse_ref, rev_ref, km_ref, dq_ref, dk_ref, dv_ref, db_ref, dk_acc, dv_acc
):
    count = q_ref.shape[0]
    width = q_ref.shape[1]
    lane = lax.broadcasted_iota(jnp.int32, (1, width), 1)
    first = lane < width // 2
    scale = (width // 2) ** (-0.5)
    zero = jnp.zeros((), bf16)
    biases = [head_tiles(rev_ref, hh) for hh in range(2)]
    near = [[None, None, None] for _ in range(2)]
    for qb in reversed(range(count // tile)):
        rows = slice(qb * tile, (qb + 1) * tile)
        keys = (qb + 1) * tile
        dq, dk, dv = 0.0, 0.0, 0.0
        for hh in range(2):
            mine = first if hh == 0 else jnp.logical_not(first)
            q_part = jnp.where(mine, q_ref[rows, :] * jnp.asarray(scale, bf16), zero)
            do_part = jnp.where(mine, do_ref[rows, :], zero)
            lse = lse_ref[0, rows, hh * (width // 2) : hh * (width // 2) + 1]
            parts = score_tiles(q_part, k_ref, km_ref, biases[hh], qb, count)
            dp = mm(do_part, v_ref[0:keys, :], 1, 1)
            probs = [jnp.exp(part - lse) for part in parts]
            dps = [dp[:, kb * tile : (kb + 1) * tile] for kb in range(qb + 1)]
            prods = [p * d for p, d in zip(probs, dps)]
            mean = jnp.sum(functools.reduce(jnp.add, prods), axis=1, keepdims=True)
            ds = [(p * (d - mean)).astype(bf16) for p, d in zip(probs, dps)]
            for kb in range(qb + 1):
                gap = min(qb - kb, 2)
                wide = ds[kb].astype(f32)
                near[hh][gap] = wide if near[hh][gap] is None else near[hh][gap] + wide
            ds_all = jnp.concatenate(ds, axis=1)
            p_all = jnp.concatenate([p.astype(bf16) for p in probs], axis=1)
            k_part = jnp.where(mine, k_ref[0:keys, :], zero)
            dq = dq + mm(ds_all, k_part)
            dk = dk + mm(ds_all, q_part, 0, 0)
            dv = dv + mm(p_all, do_part, 0, 0)
        dq_ref[rows, :] = (dq * scale).astype(bf16)
        if keys == count:
            dk_acc[...] = dk
            dv_acc[...] = dv
        else:
            dk_acc[0:keys, :] += dk
            dv_acc[0:keys, :] += dv
    dk_ref[...] = dk_acc[...].astype(bf16)
    dv_ref[...] = dv_acc[...].astype(bf16)
    for hh in range(2):
        diag, below, far = near[hh]
        if below is None:
            below = jnp.zeros_like(diag)
        line = jnp.sum(unskew(jnp.concatenate([diag, below], axis=1)), axis=0, keepdims=True)
        if far is not None:
            total = jnp.sum(far)
            spot = lax.broadcasted_iota(jnp.int32, line.shape, 1) == tile
            line = line + jnp.where(spot, total, 0.0)
        db_ref[0, hh : hh + 1, :] = line


def attention_backward(qkv, d_attn, lse, rev, key_mask):
    count, three = qkv.shape
    width = three // 3
    pairs = width // tile
    block = pl.BlockSpec((count, tile), lambda h: (0, h))
    return pl.pallas_call(
        attn_bwd_kernel,
        grid=(pairs,),
        in_specs=[
            block,
            pl.BlockSpec((count, tile), lambda h: (0, h + pairs)),
            pl.BlockSpec((count, tile), lambda h: (0, h + 2 * pairs)),
            block,
            pl.BlockSpec((1, count, tile), lambda h: (h, 0, 0)),
            pl.BlockSpec((1, 2, 2 * tile), lambda h: (h, 0, 0)),
            pl.BlockSpec((1, count), lambda h: (0, 0)),
        ],
        out_specs=[block, block, block, pl.BlockSpec((1, 2, 2 * tile), lambda h: (h, 0, 0))],
        out_shape=[jax.ShapeDtypeStruct((count, width), bf16)] * 3
        + [jax.ShapeDtypeStruct((pairs, 2, 2 * tile), f32)],
        scratch_shapes=[pltpu.VMEM((count, tile), f32), pltpu.VMEM((count, tile), f32)],
        cost_estimate=pl.CostEstimate(
            flops=10 * count * count * width, bytes_accessed=20 * count * width, transcendentals=0
        ),
        name="attn_bwd",
    )(qkv, qkv, qkv, d_attn, lse, rev, key_mask)


def expert_kernel(
    own_ref, x_ref, g_ref, other_ref, win_ref, wout_ref, wr_ref,
    made_ref, drow_ref, act_ref, dpre_ref, dmade_ref, sel_ref, made_acc, drow_acc,
):
    ff = win_ref.shape[1]
    step = 1024
    experts = wr_ref.shape[1] // 2
    x = x_ref[...]
    g = g_ref[...]
    rows = x.shape[0]
    logits = mm(x, wr_ref[...])
    ids = lax.broadcasted_iota(jnp.int32, logits.shape, 1)
    own = own_ref[0]
    other = other_ref[...]
    hit_own = ids == own
    hit_other = ids == other
    diff = jnp.sum(jnp.where(hit_other, logits, 0.0) - jnp.where(hit_own, logits, 0.0), axis=1, keepdims=True)
    pair_own = 1.0 / (1.0 + jnp.exp(diff))
    pair_other = 1.0 / (1.0 + jnp.exp(-diff))
    g_wide = g.astype(f32)
    d_made = (pair_own * g_wide).astype(bf16)
    dmade_ref[...] = d_made

    def body(i, carry):
        cols = pl.ds(pl.multiple_of(i * step, step), step)
        u = mm(x, win_ref[:, cols])
        da = mm(d_made, wout_ref[:, cols])
        u2 = u * u
        h = 0.5 + 0.5 * jnp.tanh(u * (gelu_c + (gelu_c * gelu_k) * u2))
        act = (u * h).astype(bf16)
        slope = h + u * (2.0 * gelu_c + (6.0 * gelu_c * gelu_k) * u2) * (h - h * h)
        dpre = (da * slope).astype(bf16)
        act_ref[:, cols] = act
        dpre_ref[:, cols] = dpre
        m = mm(act, wout_ref[:, cols], 1, 1)
        d = mm(dpre, win_ref[:, cols], 1, 1)

        @pl.when(i == 0)
        def _():
            made_acc[...] = m
            drow_acc[...] = d

        @pl.when(i > 0)
        def _():
            made_acc[...] += m
            drow_acc[...] += d

        return carry

    lax.fori_loop(0, ff // step, body, 0)
    made = made_acc[...].astype(bf16).astype(f32)
    made_ref[...] = (pair_own * made).astype(bf16)
    d_gate = jnp.sum(g_wide * made, axis=1, keepdims=True)
    push = pair_own * pair_other * d_gate
    full = jnp.where(hit_own, push, 0.0) - jnp.where(hit_other, push, 0.0)
    coarse = full.astype(bf16)
    fine = (full - coarse.astype(f32)).astype(bf16)
    lanes = wr_ref.shape[1]
    fine_moved = pltpu.roll(fine.astype(f32), lanes // 2, 1)
    sel = coarse.astype(f32) + fine_moved
    sel = sel.astype(bf16)
    sel_ref[...] = sel
    back = mm(coarse, wr_ref[...], 1, 1)
    drow_ref[...] = (drow_acc[...] + back).astype(bf16)


def expert_pass(own, x_rows, g_rows, other, w_in, w_out, w_router):
    rows, width = x_rows.shape
    ff = w_in.shape[1]
    rt = 256
    lanes = w_router.shape[1]
    row_block = pl.BlockSpec((rt, width), lambda r: (r, 0))
    ff_block = pl.BlockSpec((rt, ff), lambda r: (r, 0))
    once = dict(pipeline_mode=pl.Buffered(1))
    return pl.pallas_call(
        expert_kernel,
        grid=(rows // rt,),
        in_specs=[
            pl.BlockSpec(memory_space=pltpu.SMEM),
            row_block,
            row_block,
            pl.BlockSpec((rt, 1), lambda r: (r, 0)),
            pl.BlockSpec((width, ff), lambda r: (0, 0), **once),
            pl.BlockSpec((width, ff), lambda r: (0, 0), **once),
            pl.BlockSpec((width, lanes), lambda r: (0, 0), **once),
        ],
        out_specs=[row_block, row_block, ff_block, ff_block, row_block, pl.BlockSpec((rt, lanes), lambda r: (r, 0))],
        out_shape=[
            jax.ShapeDtypeStruct((rows, width), bf16),
            jax.ShapeDtypeStruct((rows, width), bf16),
            jax.ShapeDtypeStruct((rows, ff), bf16),
            jax.ShapeDtypeStruct((rows, ff), bf16),
            jax.ShapeDtypeStruct((rows, width), bf16),
            jax.ShapeDtypeStruct((rows, lanes), bf16),
        ],
        scratch_shapes=[pltpu.VMEM((rt, width), f32), pltpu.VMEM((rt, width), f32)],
        compiler_params=pltpu.CompilerParams(vmem_limit_bytes=56 << 20),
        cost_estimate=pl.CostEstimate(
            flops=8 * rows * width * ff, bytes_accessed=4 * rows * ff + 4 * width * ff, transcendentals=0
        ),
        name="expert_pass",
    )(own, x_rows, g_rows, other, w_in, w_out, w_router)


def weight_grad_kernel(x_ref, dm_ref, act_ref, dpre_ref, gin_ref, gout_ref):
    gout_ref[...] = mm(dm_ref[...], act_ref[...], 0, 0).astype(bf16)
    gin_ref[...] = mm(x_ref[...], dpre_ref[...], 0, 0).astype(bf16)


def weight_grads(x_rows, d_made, act, d_pre):
    rows, width = x_rows.shape
    ff = act.shape[1]
    ft = 512
    full = pl.BlockSpec((rows, width), lambda f: (0, 0), pipeline_mode=pl.Buffered(1))
    cols = pl.BlockSpec((rows, ft), lambda f: (0, f))
    outs = pl.BlockSpec((width, ft), lambda f: (0, f))
    return pl.pallas_call(
        weight_grad_kernel,
        grid=(ff // ft,),
        in_specs=[full, full, cols, cols],
        out_specs=[outs, outs],
        out_shape=[jax.ShapeDtypeStruct((width, ff), bf16)] * 2,
        compiler_params=pltpu.CompilerParams(vmem_limit_bytes=56 << 20),
        cost_estimate=pl.CostEstimate(
            flops=4 * rows * width * ff, bytes_accessed=4 * rows * ff + 4 * width * ff, transcendentals=0
        ),
        name="weight_grads",
    )(x_rows, d_made, act, d_pre)


def rms_scale(vector):
    return lax.rsqrt(jnp.mean(vector * vector, axis=-1, keepdims=True) + norm_eps)


def rms_back(vector, scale, gain_vec, cotangent):
    inner = cotangent * gain_vec
    push = jnp.mean(inner * vector, axis=-1, keepdims=True)
    d_vector = scale * inner - vector * (scale * scale * scale) * push
    d_gain = jnp.sum(cotangent * (vector * scale), axis=0)
    return d_vector, d_gain


def on_device(
    inputs, cotangent, lengths, routes, w_qkv, w_attn_out, w_router,
    gain_attn, gain_moe, rel_bias, w_in, w_out,
):
    tok_count, model_width = inputs.shape
    group = lax.axis_size("expert")
    dp_count = lax.axis_size("dp")
    shard = w_qkv.shape[0]
    head_count = rel_bias.shape[0] * dp_count
    bucket_count = rel_bias.shape[1]
    expert_count = w_router.shape[1]
    assert w_in.shape[0] == 1 and expert_count == group and routes.shape[1] == 2
    capacity = round_up(3 * tok_count * 2 // (2 * expert_count), 32)
    rows = expert_count * capacity

    bias_cells = rel_bias.size
    small = jnp.concatenate(
        [
            w_router,
            gain_attn[:, None],
            gain_moe[:, None],
            jnp.pad(rel_bias.reshape(-1), (0, shard - bias_cells))[:, None],
        ],
        axis=1,
    )
    small = jnp.pad(small, ((0, 0), (0, tile - small.shape[1])))
    gathered = lax.all_gather(jnp.concatenate([w_qkv, small], axis=1), "dp", axis=0, tiled=True)
    w_mix = lax.all_gather(w_attn_out, "dp", axis=0, tiled=True)
    w_proj = gathered[:, : 3 * model_width]
    small_all = gathered[:, 3 * model_width :]
    w_gate = small_all[:, :expert_count]
    gain_first = small_all[:, expert_count].astype(f32)
    gain_second = small_all[:, expert_count + 1].astype(f32)
    bias_table = small_all[:, expert_count + 2].reshape(dp_count, shard)[:, :bias_cells]
    bias_table = bias_table.reshape(head_count, bucket_count)

    positions = jnp.arange(tok_count, dtype=jnp.int32)
    valid = positions < lengths[0]
    valid_mask = valid.astype(f32)[:, None]
    expert_ids = jnp.arange(expert_count, dtype=jnp.int32)
    hot = jnp.any(routes[:, :, None] == expert_ids, axis=1) & valid[:, None]
    hot_b = hot.astype(bf16)
    lower = (positions[:, None] > positions[None, :]).astype(bf16)
    rank = jnp.dot(lower, hot_b, preferred_element_type=f32).astype(jnp.int32)
    rank = jnp.where(hot, rank, -1)
    slots = jnp.arange(capacity, dtype=jnp.int32)
    select = (rank.T[:, None, :] == slots[None, :, None]).astype(bf16).reshape(rows, tok_count)
    both = jnp.sum(routes, axis=1)
    other_tok = (both[:, None] - expert_ids[None, :]) * hot.astype(jnp.int32) - (1 - hot.astype(jnp.int32))
    chosen = rank.T[:, None, :] == slots[None, :, None]
    other_slot = jnp.sum(jnp.where(chosen, both[None, None, :], 0), axis=2) - expert_ids[:, None]

    def to_experts(block):
        return lax.all_to_all(
            block.reshape((group, capacity) + block.shape[1:]), "expert", split_axis=0, concat_axis=0, tiled=True
        ).reshape(block.shape)

    g_rows = to_experts(jnp.dot(select, cotangent, preferred_element_type=f32).astype(bf16))
    other = to_experts(other_slot.reshape(rows, 1))

    distances = (2 * tile - jnp.arange(2 * tile, dtype=jnp.int32)) % (2 * tile)
    bucket_hot = (bucket_of(distances)[:, None] == jnp.arange(bucket_count)).astype(f32)
    rev = jnp.sum(bias_table.astype(f32)[:, None, :] * bucket_hot[None], axis=-1)
    rev = rev.reshape(head_count // 2, 2, 2 * tile)
    key_mask = jnp.where(valid, 0.0, neg_big)[None, :].astype(f32)
    inputs_wide = inputs.astype(f32)
    scale_first = rms_scale(inputs_wide)
    normed_attn = (inputs_wide * scale_first * gain_first).astype(bf16)
    qkv = jnp.dot(normed_attn, w_proj, preferred_element_type=f32).astype(bf16)
    attn_heads, lse = attention_forward(qkv, rev, key_mask)
    hidden = inputs_wide + valid_mask * jnp.dot(attn_heads, w_mix, preferred_element_type=f32)
    scale_second = rms_scale(hidden)
    normed_moe = (hidden * scale_second * gain_second).astype(bf16)

    x_rows = to_experts(jnp.dot(select, normed_moe, preferred_element_type=f32).astype(bf16))
    lanes = max(tile, 2 * expert_count)
    w_gate_wide = jnp.zeros((model_width, lanes), bf16).at[:, :expert_count].set(w_gate)
    own = lax.axis_index("expert").astype(jnp.int32).reshape(1)
    made, d_rows, act, d_pre, d_made, sel = expert_pass(
        own, x_rows, g_rows, other, w_in[0], w_out[0], w_gate_wide
    )
    d_back = to_experts(d_rows)
    made_back = to_experts(made)
    full_in, full_out = weight_grads(x_rows, d_made, act, d_pre)
    grad_w_in = lax.psum_scatter(full_in, "dp", scatter_dimension=1, tiled=True).astype(f32)[None]
    grad_w_out = lax.psum_scatter(full_out, "dp", scatter_dimension=1, tiled=True).astype(f32)[None]
    router_wide = jnp.dot(x_rows.T, sel, preferred_element_type=f32)
    grad_router = router_wide[:, :expert_count] + router_wide[:, lanes // 2 : lanes // 2 + expert_count]

    moe_out = jnp.dot(select.T, made_back, preferred_element_type=f32)
    outputs = (valid_mask * (hidden + moe_out)).astype(bf16)

    d_normed = jnp.dot(select.T, d_back, preferred_element_type=f32)
    d_hidden_norm, grad_gain_moe = rms_back(hidden, scale_second, gain_second, d_normed)
    d_hidden = cotangent.astype(f32) * valid_mask + d_hidden_norm
    d_proj = (d_hidden * valid_mask).astype(bf16)
    grad_attn_out = jnp.dot(attn_heads.T, d_proj, preferred_element_type=f32)
    d_heads = jnp.dot(d_proj, w_mix.T, preferred_element_type=f32).astype(bf16)
    dq, dk, dv, d_line = attention_backward(qkv, d_heads, lse, rev, key_mask)
    d_qkv = jnp.concatenate([dq, dk, dv], axis=1)
    near = jnp.arange(2 * tile, dtype=jnp.int32)
    line_hot = (bucket_of((2 * tile - near) % (2 * tile))[:, None] == jnp.arange(bucket_count)).astype(f32)
    grad_rel_bias = jnp.sum(d_line.reshape(head_count, 2 * tile, 1) * line_hot[None], axis=1)
    grad_qkv = jnp.dot(normed_attn.T, d_qkv, preferred_element_type=f32)
    d_normed_attn = jnp.dot(d_qkv, w_proj.T, preferred_element_type=f32)
    d_norm_in, grad_gain_attn = rms_back(inputs_wide, scale_first, gain_first, d_normed_attn)
    d_inputs = (d_hidden + d_norm_in).astype(bf16)

    bias_col = jnp.pad(
        grad_rel_bias.reshape(dp_count, bias_cells), ((0, 0), (0, shard - bias_cells))
    ).reshape(model_width, 1)
    small_grad = jnp.concatenate(
        [grad_router, grad_gain_attn[:, None], grad_gain_moe[:, None], bias_col], axis=1
    )
    small_grad = jnp.pad(small_grad, ((0, 0), (0, tile - small_grad.shape[1])))
    packed = jnp.concatenate([grad_qkv, grad_attn_out, small_grad], axis=1).astype(bf16)
    part = lax.psum_scatter(packed, "dp", scatter_dimension=0, tiled=True)
    whole = lax.psum(part, "expert").astype(f32)
    end = 4 * model_width
    tail = whole[:, end:]
    return (
        outputs,
        d_inputs,
        whole[:, : 3 * model_width],
        whole[:, 3 * model_width : end],
        tail[:, :expert_count],
        tail[:, expert_count],
        tail[:, expert_count + 1],
        tail[:bias_cells, expert_count + 2].reshape(rel_bias.shape),
        grad_w_in,
        grad_w_out,
    )


def solution(mesh):
    placed = (
        P(("dp", "expert"), None),
        P(("dp", "expert"), None),
        P(("dp", "expert")),
        P(("dp", "expert"), None),
        P("dp", None),
        P("dp", None),
        P("dp", None),
        P("dp"),
        P("dp"),
        P("dp", None),
        P("expert", None, None),
        P("expert", None, None),
    )
    return jax.shard_map(
        on_device,
        mesh=mesh,
        in_specs=placed,
        out_specs=(
            P(("dp", "expert"), None),
            P(("dp", "expert"), None),
            P("dp", None),
            P("dp", None),
            P("dp", None),
            P("dp"),
            P("dp"),
            P("dp", None),
            P("expert", None, "dp"),
            P("expert", None, "dp"),
        ),
        check_vma=False,
    )
```

```python
import functools
import math

import jax
import jax.numpy as jnp
from jax import lax
from jax.experimental import pallas as pl
from jax.experimental.pallas import tpu as pltpu
from jax.sharding import PartitionSpec as P

norm_eps = 1e-06
rel_edges = (19, 21, 24, 27, 31, 35, 40, 46, 52, 59, 67, 77, 87, 99, 113)
far_start = 113
bf16 = jnp.bfloat16
f32 = jnp.float32
neg_big = -1e30
tile = 128
gelu_c = math.sqrt(2.0 / math.pi)
gelu_k = 0.044715


def bucket_of(distance):
    far_bucket = jnp.full(distance.shape, 16, jnp.int32)
    for edge_value in rel_edges:
        far_bucket = far_bucket + (distance >= edge_value).astype(jnp.int32)
    return jnp.where(distance < 16, distance, far_bucket)


def mm(a, b, ca=1, cb=0):
    return lax.dot_general(a, b, (((ca,), (cb,)), ((), ())), preferred_element_type=f32)


def round_up(a, b):
    return (a + b - 1) // b * b


def head_tiles(rev_ref, hh):
    row = rev_ref[0, hh : hh + 1, :]
    toe = pltpu.roll(jnp.broadcast_to(row, (tile, 2 * tile)), 0, 1, stride=1, stride_axis=0)
    down = lax.broadcasted_iota(jnp.int32, (tile, tile), 0)
    across = lax.broadcasted_iota(jnp.int32, (tile, tile), 1)
    diag = jnp.where(down >= across, toe[:, :tile], neg_big)
    return diag, toe[:, tile:], jnp.broadcast_to(row[:, tile : tile + 1], (tile, tile))


def score_tiles(q_part, k_ref, km_ref, bias, qb, count):
    keys = (qb + 1) * tile
    raw = mm(q_part, k_ref[0:keys, :], 1, 1)
    out = []
    for kb in range(qb + 1):
        part = raw[:, kb * tile : (kb + 1) * tile] + bias[min(qb - kb, 2)]
        if (kb + 1) * tile > 3 * count // 4:
            part = part + km_ref[0:1, kb * tile : (kb + 1) * tile]
        out.append(part)
    return out


def attn_fwd_kernel(q_ref, k_ref, v_ref, rev_ref, km_ref, o_ref, lse_ref):
    count = q_ref.shape[0]
    width = q_ref.shape[1]
    lane = lax.broadcasted_iota(jnp.int32, (1, width), 1)
    first = lane < width // 2
    scale = jnp.asarray((width // 2) ** (-0.5), bf16)
    biases = [head_tiles(rev_ref, hh) for hh in range(2)]
    for qb in range(count // tile):
        rows = slice(qb * tile, (qb + 1) * tile)
        outs, lses = [], []
        for hh in range(2):
            mine = first if hh == 0 else jnp.logical_not(first)
            q_part = jnp.where(mine, q_ref[rows, :] * scale, jnp.zeros((), bf16))
            parts = score_tiles(q_part, k_ref, km_ref, biases[hh], qb, count)
            top = functools.reduce(jnp.maximum, parts)
            top = jnp.max(top, axis=1, keepdims=True)
            exps = [jnp.exp(part - top) for part in parts]
            total = jnp.sum(functools.reduce(jnp.add, exps), axis=1, keepdims=True)
            inv = 1.0 / total
            probs = jnp.concatenate([(e * inv).astype(bf16) for e in exps], axis=1)
            outs.append(mm(probs, v_ref[0 : (qb + 1) * tile, :]))
            lses.append(top + jnp.log(total))
        o_ref[rows, :] = jnp.where(first, outs[0], outs[1]).astype(bf16)
        lse_ref[0, rows, :] = jnp.where(first, lses[0], lses[1])


def attention_forward(qkv, rev, key_mask):
    count, three = qkv.shape
    width = three // 3
    pairs = width // tile
    return pl.pallas_call(
        attn_fwd_kernel,
        grid=(pairs,),
        in_specs=[
            pl.BlockSpec((count, tile), lambda h: (0, h)),
            pl.BlockSpec((count, tile), lambda h: (0, h + pairs)),
            pl.BlockSpec((count, tile), lambda h: (0, h + 2 * pairs)),
            pl.BlockSpec((1, 2, 2 * tile), lambda h: (h, 0, 0)),
            pl.BlockSpec((1, count), lambda h: (0, 0)),
        ],
        out_specs=[
            pl.BlockSpec((count, tile), lambda h: (0, h)),
            pl.BlockSpec((1, count, tile), lambda h: (h, 0, 0)),
        ],
        out_shape=[
            jax.ShapeDtypeStruct((count, width), bf16),
            jax.ShapeDtypeStruct((pairs, count, tile), f32),
        ],
        cost_estimate=pl.CostEstimate(
            flops=4 * count * count * width, bytes_accessed=16 * count * width, transcendentals=0
        ),
        name="attn_fwd",
    )(qkv, qkv, qkv, rev, key_mask)


def unskew(block):
    down = lax.broadcasted_iota(jnp.int32, block.shape, 0)
    lanes = block.shape[1]
    step = 1
    while step < block.shape[0]:
        moved = pltpu.roll(block, lanes - step, 1)
        block = jnp.where((down & step) != 0, moved, block)
        step *= 2
    return block


def attn_bwd_kernel(
    q_ref, k_ref, v_ref, do_ref, lse_ref, rev_ref, km_ref, dq_ref, dk_ref, dv_ref, db_ref, dk_acc, dv_acc
):
    count = q_ref.shape[0]
    width = q_ref.shape[1]
    lane = lax.broadcasted_iota(jnp.int32, (1, width), 1)
    first = lane < width // 2
    scale = (width // 2) ** (-0.5)
    zero = jnp.zeros((), bf16)
    biases = [head_tiles(rev_ref, hh) for hh in range(2)]
    near = [[None, None, None] for _ in range(2)]
    for qb in reversed(range(count // tile)):
        rows = slice(qb * tile, (qb + 1) * tile)
        keys = (qb + 1) * tile
        dq, dk, dv = 0.0, 0.0, 0.0
        for hh in range(2):
            mine = first if hh == 0 else jnp.logical_not(first)
            q_part = jnp.where(mine, q_ref[rows, :] * jnp.asarray(scale, bf16), zero)
            do_part = jnp.where(mine, do_ref[rows, :], zero)
            lse = lse_ref[0, rows, hh * (width // 2) : hh * (width // 2) + 1]
            parts = score_tiles(q_part, k_ref, km_ref, biases[hh], qb, count)
            dp = mm(do_part, v_ref[0:keys, :], 1, 1)
            probs = [jnp.exp(part - lse) for part in parts]
            dps = [dp[:, kb * tile : (kb + 1) * tile] for kb in range(qb + 1)]
            prods = [p * d for p, d in zip(probs, dps)]
            mean = jnp.sum(functools.reduce(jnp.add, prods), axis=1, keepdims=True)
            ds = [(p * (d - mean)).astype(bf16) for p, d in zip(probs, dps)]
            for kb in range(qb + 1):
                gap = min(qb - kb, 2)
                wide = ds[kb].astype(f32)
                near[hh][gap] = wide if near[hh][gap] is None else near[hh][gap] + wide
            ds_all = jnp.concatenate(ds, axis=1)
            p_all = jnp.concatenate([p.astype(bf16) for p in probs], axis=1)
            k_part = jnp.where(mine, k_ref[0:keys, :], zero)
            dq = dq + mm(ds_all, k_part)
            dk = dk + mm(ds_all, q_part, 0, 0)
            dv = dv + mm(p_all, do_part, 0, 0)
        dq_ref[rows, :] = (dq * scale).astype(bf16)
        if keys == count:
            dk_acc[...] = dk
            dv_acc[...] = dv
        else:
            dk_acc[0:keys, :] += dk
            dv_acc[0:keys, :] += dv
    dk_ref[...] = dk_acc[...].astype(bf16)
    dv_ref[...] = dv_acc[...].astype(bf16)
    for hh in range(2):
        diag, below, far = near[hh]
        if below is None:
            below = jnp.zeros_like(diag)
        line = jnp.sum(unskew(jnp.concatenate([diag, below], axis=1)), axis=0, keepdims=True)
        if far is not None:
            total = jnp.sum(far)
            spot = lax.broadcasted_iota(jnp.int32, line.shape, 1) == tile
            line = line + jnp.where(spot, total, 0.0)
        db_ref[0, hh : hh + 1, :] = line


def attention_backward(qkv, d_attn, lse, rev, key_mask):
    count, three = qkv.shape
    width = three // 3
    pairs = width // tile
    block = pl.BlockSpec((count, tile), lambda h: (0, h))
    return pl.pallas_call(
        attn_bwd_kernel,
        grid=(pairs,),
        in_specs=[
            block,
            pl.BlockSpec((count, tile), lambda h: (0, h + pairs)),
            pl.BlockSpec((count, tile), lambda h: (0, h + 2 * pairs)),
            block,
            pl.BlockSpec((1, count, tile), lambda h: (h, 0, 0)),
            pl.BlockSpec((1, 2, 2 * tile), lambda h: (h, 0, 0)),
            pl.BlockSpec((1, count), lambda h: (0, 0)),
        ],
        out_specs=[block, block, block, pl.BlockSpec((1, 2, 2 * tile), lambda h: (h, 0, 0))],
        out_shape=[jax.ShapeDtypeStruct((count, width), bf16)] * 3
        + [jax.ShapeDtypeStruct((pairs, 2, 2 * tile), f32)],
        scratch_shapes=[pltpu.VMEM((count, tile), f32), pltpu.VMEM((count, tile), f32)],
        cost_estimate=pl.CostEstimate(
            flops=10 * count * count * width, bytes_accessed=20 * count * width, transcendentals=0
        ),
        name="attn_bwd",
    )(qkv, qkv, qkv, d_attn, lse, rev, key_mask)


def remote(src, dst, send, recv, dp, expert):
    return pltpu.make_async_remote_copy(
        src_ref=src, dst_ref=dst, send_sem=send, recv_sem=recv,
        device_id={"dp": dp, "expert": expert}, device_id_type=pl.DeviceIdType.MESH,
    )


def greet(dp, expert, group, across):
    barrier = pltpu.get_barrier_semaphore()

    def hello(dp_to, expert_to):
        pl.semaphore_signal(
            barrier, inc=1, device_id={"dp": dp_to, "expert": expert_to}, device_id_type=pl.DeviceIdType.MESH
        )

    def one(k, carry):
        hello(dp, lax.rem(expert + k, group))
        return carry

    lax.fori_loop(1, group, one, 0)
    for flip in across:
        hello(flipped(dp, flip), expert)
    pl.semaphore_wait(barrier, group - 1 + len(across))


def flipped(dp, flip):
    low = lax.rem(dp, 2)
    high = dp - low
    if flip & 1:
        low = 1 - low
    if flip & 2:
        high = 2 - high
    return high + low


def expert_kernel(
    xb_ref, sel_ref, other_ref, wr_ref, g_hbm, win_hbm, wout_hbm,
    dnorm_ref, made_hbm, gin_hbm, gout_ref, router_ref,
    xs, xr, gr, db, win, wout, act, dpre, drow_acc, stage,
    s_diag, s_x, s_y, r1x, r1y, r2x, r2y,
    x_send, x_recv, d_send, d_recv, r_send, r_recv, load_sem, made_sem, out_sem,
    *, group, chunks, step,
):
    dp = lax.axis_index("dp")
    me = lax.axis_index("expert")
    width = xb_ref.shape[1]
    ff = win.shape[1]
    made_acc = dnorm_ref
    cap = xs.shape[1]
    cs = cap // chunks
    rows = group * cs

    loads = [
        pltpu.make_async_copy(g_hbm, gr, load_sem.at[0]),
        pltpu.make_async_copy(win_hbm, win, load_sem.at[1]),
        pltpu.make_async_copy(wout_hbm, wout, load_sem.at[2]),
    ]
    for load in loads:
        load.start()

    def part(c):
        return pl.ds(pl.multiple_of(c * cs, cs), cs)

    def x_copy(c, k):
        to = lax.rem(me + k, group)
        return remote(xs.at[to, part(c)], xr.at[me, part(c)], x_send.at[c, k], x_recv.at[c, k], dp, to)

    def d_copy(c, k):
        to = lax.rem(me + k, group)
        return remote(xs.at[to, part(c)], db.at[me, part(c)], d_send.at[c, k], d_recv.at[c, k], dp, to)

    def over_peers(f):
        def one(k, carry):
            f(k)
            return carry

        lax.fori_loop(1, group, one, 0)

    def made_copy(c, k):
        src = s_x.at[pl.ds(pl.multiple_of(k * cs, cs), cs)]
        return pltpu.make_async_copy(src, made_hbm.at[k, part(c)], made_sem.at[k])

    def over_all(f):
        def one(k, carry):
            f(k)
            return carry

        lax.fori_loop(0, group, one, 0)

    def pick(c, carry):
        chosen = sel_ref[:, part(c), :].reshape(rows, sel_ref.shape[2])
        xs[:, part(c), :] = mm(chosen, xb_ref[...]).astype(bf16).reshape(group, cs, width)

        @pl.when(c == 0)
        def _():
            greet(dp, me, group, (1, 2))

        over_peers(lambda k: x_copy(c, k).start())
        xr[me, part(c), :] = xs[me, part(c), :]
        return carry

    lax.fori_loop(0, chunks, pick, 0)
    for load in loads:
        load.wait()
    router_ref[...] = jnp.zeros_like(router_ref)

    def work(c, carry):
        over_peers(lambda k: x_copy(c, k).wait())
        x = xr[:, part(c), :].reshape(rows, width)
        g_wide = gr[:, part(c), :].reshape(rows, width).astype(f32)
        logits = mm(x, wr_ref[...])
        ids = lax.broadcasted_iota(jnp.int32, logits.shape, 1)
        hit_own = ids == me
        hit_other = ids == other_ref[:, part(c), :].reshape(rows, 1)
        diff = jnp.sum(
            jnp.where(hit_other, logits, 0.0) - jnp.where(hit_own, logits, 0.0), axis=1, keepdims=True
        )
        pair_own = 1.0 / (1.0 + jnp.exp(diff))
        pair_other = 1.0 / (1.0 + jnp.exp(-diff))
        d_made = (pair_own * g_wide).astype(bf16)

        def body(i, inner):
            cols = pl.ds(pl.multiple_of(i * step, step), step)
            u = mm(x, win[:, cols])
            da = mm(d_made, wout[:, cols])
            u2 = u * u
            h = 0.5 + 0.5 * jnp.tanh(u * (gelu_c + (gelu_c * gelu_k) * u2))
            a = (u * h).astype(bf16)
            slope = h + u * (2.0 * gelu_c + (6.0 * gelu_c * gelu_k) * u2) * (h - h * h)
            d = (da * slope).astype(bf16)
            act[:, part(c), cols] = a.reshape(group, cs, step)
            dpre[:, part(c), cols] = d.reshape(group, cs, step)
            m_part = mm(a, wout[:, cols], 1, 1)
            d_part = mm(d, win[:, cols], 1, 1)

            @pl.when(i == 0)
            def _():
                made_acc[...] = m_part
                drow_acc[...] = d_part

            @pl.when(i > 0)
            def _():
                made_acc[...] += m_part
                drow_acc[...] += d_part

            return inner

        lax.fori_loop(0, ff // step, body, 0)
        made = made_acc[...].astype(bf16).astype(f32)
        d_gate = jnp.sum(g_wide * made, axis=1, keepdims=True)
        push = pair_own * pair_other * d_gate
        full = jnp.where(hit_own, push, 0.0) - jnp.where(hit_other, push, 0.0)
        coarse = full.astype(bf16)
        fine = full - coarse.astype(f32)
        lanes = wr_ref.shape[1]
        spread = (coarse.astype(f32) + pltpu.roll(fine, lanes // 2, 1)).astype(bf16)
        router_ref[...] += mm(x, spread, 0, 0)
        d_row = (drow_acc[...] + mm(coarse, wr_ref[...], 1, 1)).astype(bf16)
        xs[:, part(c), :] = d_row.reshape(group, cs, width)
        over_peers(lambda k: d_copy(c, k).start())
        db[me, part(c), :] = xs[me, part(c), :]

        @pl.when(c > 0)
        def _():
            over_all(lambda k: made_copy(c - 1, k).wait())

        s_x[0:rows, :] = (pair_own * made).astype(bf16)
        over_all(lambda k: made_copy(c, k).start())
        gr[:, part(c), :] = d_made.reshape(group, cs, width)
        return carry

    lax.fori_loop(0, chunks, work, 0)
    over_all(lambda k: made_copy(chunks - 1, k).wait())

    total_rows = group * cap
    shard = ff // 4
    half = width // 2
    piece = shard // 2

    def grad_cols(left, right, start):
        a = left[...].reshape(total_rows, width)
        b = right[:, :, pl.ds(start, piece)].reshape(total_rows, piece)
        return mm(a, b, 0, 0)

    def shard_into(dst, owner):
        for p in range(2):
            start = pl.multiple_of(owner * shard + p * piece, piece)
            dst[:, p * piece : (p + 1) * piece] = grad_cols(gr, act, start).astype(dst.dtype)

    px, py, pd = flipped(dp, 1), flipped(dp, 2), flipped(dp, 3)
    upper, lower = slice(0, half), slice(half, width)
    to_x1 = remote(s_diag.at[upper], r1x, r_send.at[0], r_recv.at[0], px, me)
    to_y1 = remote(s_diag.at[lower], r1y, r_send.at[1], r_recv.at[1], py, me)
    to_xa = remote(s_x.at[upper], r2x.at[upper], r_send.at[2], r_recv.at[2], px, me)
    to_xb = remote(s_x.at[lower], r2x.at[lower], r_send.at[3], r_recv.at[3], px, me)
    to_ya = remote(s_y.at[upper], r2y.at[upper], r_send.at[4], r_recv.at[4], py, me)
    to_yb = remote(s_y.at[lower], r2y.at[lower], r_send.at[5], r_recv.at[5], py, me)
    shard_into(s_diag, pd)
    to_x1.start()
    to_y1.start()
    shard_into(s_x, px)
    to_xa.start()
    shard_into(s_y, py)
    to_yb.start()

    def out_copy(i):
        slot = lax.rem(i, 2)
        cols = pl.ds(pl.multiple_of(i * piece, piece), piece)
        return pltpu.make_async_copy(stage.at[slot], gin_hbm.at[:, cols], out_sem.at[slot])

    def in_grad(i, carry):
        @pl.when(i >= 2)
        def _():
            out_copy(i - 2).wait()

        x_all = xr[...].reshape(total_rows, width)
        cols = pl.ds(pl.multiple_of(i * piece, piece), piece)
        stage[lax.rem(i, 2)] = mm(x_all, dpre[:, :, cols].reshape(total_rows, piece), 0, 0).astype(bf16)
        out_copy(i).start()
        return carry

    lax.fori_loop(0, 4, in_grad, 0)
    to_y1.wait()
    s_x[lower, :] = (s_x[lower, :].astype(f32) + r1y[...].astype(f32)).astype(bf16)
    to_xb.start()
    to_x1.wait()
    s_y[upper, :] = (s_y[upper, :].astype(f32) + r1x[...].astype(f32)).astype(bf16)
    to_ya.start()
    lax.fori_loop(4, 8, in_grad, 0)
    shard_into(gout_ref, dp)

    def all_back(c, carry):
        over_peers(lambda k: d_copy(c, k).wait())
        return carry

    lax.fori_loop(0, chunks, all_back, 0)
    dnorm_ref[...] = mm(
        sel_ref[...].reshape(total_rows, sel_ref.shape[2]), db[...].reshape(total_rows, width), 0, 0
    )
    for copy in (to_xa, to_xb, to_ya, to_yb):
        copy.wait()
    gout_ref[...] += r2x[...].astype(f32) + r2y[...].astype(f32)
    out_copy(6).wait()
    out_copy(7).wait()


def expert_pass(xb, select, other, w_router, g_rows, w_in, w_out, chunks):
    group, cap, tok_count = select.shape
    width = xb.shape[1]
    ff = w_in.shape[1]
    cs = cap // chunks
    rows = group * cs
    lanes = w_router.shape[1]
    shard = ff // 4
    assert rows == tok_count and rows <= width
    vmem = pl.BlockSpec(memory_space=pltpu.VMEM)
    hbm = pl.BlockSpec(memory_space=pl.ANY)
    block = (group, cap, width)
    dma = pltpu.SemaphoreType.DMA
    return pl.pallas_call(
        functools.partial(expert_kernel, group=group, chunks=chunks, step=512),
        in_specs=[vmem, vmem, vmem, vmem, hbm, hbm, hbm],
        out_specs=[vmem, hbm, hbm, vmem, vmem],
        out_shape=[
            jax.ShapeDtypeStruct((tok_count, width), f32),
            jax.ShapeDtypeStruct(block, bf16),
            jax.ShapeDtypeStruct((width, ff), bf16),
            jax.ShapeDtypeStruct((width, shard), f32),
            jax.ShapeDtypeStruct((width, lanes), f32),
        ],
        scratch_shapes=[
            pltpu.VMEM(block, bf16),
            pltpu.VMEM(block, bf16),
            pltpu.VMEM(block, bf16),
            pltpu.VMEM(block, bf16),
            pltpu.VMEM((width, ff), bf16),
            pltpu.VMEM((width, ff), bf16),
            pltpu.VMEM((group, cap, ff), bf16),
            pltpu.VMEM((group, cap, ff), bf16),
            pltpu.VMEM((rows, width), f32),
            pltpu.VMEM((2, width, shard // 2), bf16),
            pltpu.VMEM((width, shard), bf16),
            pltpu.VMEM((width, shard), bf16),
            pltpu.VMEM((width, shard), bf16),
            pltpu.VMEM((width // 2, shard), bf16),
            pltpu.VMEM((width // 2, shard), bf16),
            pltpu.VMEM((width, shard), bf16),
            pltpu.VMEM((width, shard), bf16),
            dma((chunks, group)),
            dma((chunks, group)),
            dma((chunks, group)),
            dma((chunks, group)),
            dma((6,)),
            dma((6,)),
            dma((3,)),
            dma((group,)),
            dma((2,)),
        ],
        compiler_params=pltpu.CompilerParams(
            collective_id=1, has_side_effects=True, vmem_limit_bytes=67_000_000
        ),
        cost_estimate=pl.CostEstimate(
            flops=12 * group * cap * width * ff, bytes_accessed=8 * width * ff, transcendentals=0
        ),
        name="expert_pass",
    )(xb, select, other, w_router, g_rows, w_in, w_out)


def rms_scale(vector):
    return lax.rsqrt(jnp.mean(vector * vector, axis=-1, keepdims=True) + norm_eps)


def rms_back(vector, scale, gain_vec, cotangent):
    inner = cotangent * gain_vec
    push = jnp.mean(inner * vector, axis=-1, keepdims=True)
    d_vector = scale * inner - vector * (scale * scale * scale) * push
    d_gain = jnp.sum(cotangent * (vector * scale), axis=0)
    return d_vector, d_gain


def on_device(
    inputs, cotangent, lengths, routes, w_qkv, w_attn_out, w_router,
    gain_attn, gain_moe, rel_bias, w_in, w_out,
):
    tok_count, model_width = inputs.shape
    group = lax.axis_size("expert")
    dp_count = lax.axis_size("dp")
    shard = w_qkv.shape[0]
    head_count = rel_bias.shape[0] * dp_count
    bucket_count = rel_bias.shape[1]
    expert_count = w_router.shape[1]
    assert w_in.shape[0] == 1 and expert_count == group and routes.shape[1] == 2
    capacity = 3 * tok_count * 2 // (2 * expert_count)
    rows = expert_count * capacity

    bias_cells = rel_bias.size
    small = jnp.concatenate(
        [
            w_router,
            gain_attn[:, None],
            gain_moe[:, None],
            jnp.pad(rel_bias.reshape(-1), (0, shard - bias_cells))[:, None],
        ],
        axis=1,
    )
    small = jnp.pad(small, ((0, 0), (0, tile - small.shape[1])))
    gathered = lax.all_gather(jnp.concatenate([w_qkv, small], axis=1), "dp", axis=0, tiled=True)
    w_mix = lax.all_gather(w_attn_out, "dp", axis=0, tiled=True)
    w_proj = gathered[:, : 3 * model_width]
    small_all = gathered[:, 3 * model_width :]
    w_gate = small_all[:, :expert_count]
    gain_first = small_all[:, expert_count].astype(f32)
    gain_second = small_all[:, expert_count + 1].astype(f32)
    bias_table = small_all[:, expert_count + 2].reshape(dp_count, shard)[:, :bias_cells]
    bias_table = bias_table.reshape(head_count, bucket_count)

    positions = jnp.arange(tok_count, dtype=jnp.int32)
    valid = positions < lengths[0]
    valid_mask = valid.astype(f32)[:, None]
    expert_ids = jnp.arange(expert_count, dtype=jnp.int32)
    hot = jnp.any(routes[:, :, None] == expert_ids, axis=1) & valid[:, None]
    hot_b = hot.astype(bf16)
    lower = (positions[:, None] > positions[None, :]).astype(bf16)
    rank = jnp.dot(lower, hot_b, preferred_element_type=f32).astype(jnp.int32)
    rank = jnp.where(hot, rank, -1)
    slots = jnp.arange(capacity, dtype=jnp.int32)
    select = (rank.T[:, None, :] == slots[None, :, None]).astype(bf16).reshape(rows, tok_count)
    both = jnp.sum(routes, axis=1)
    chosen = rank.T[:, None, :] == slots[None, :, None]
    other_slot = jnp.sum(jnp.where(chosen, both[None, None, :], 0), axis=2) - expert_ids[:, None]

    def to_experts(block):
        return lax.all_to_all(block, "expert", split_axis=0, concat_axis=0, tiled=True)

    g_rows = jnp.dot(select, cotangent, preferred_element_type=f32).astype(bf16)
    g_rows = to_experts(g_rows.reshape(group, capacity, model_width))
    other = to_experts(other_slot.reshape(group, capacity, 1))

    distances = (2 * tile - jnp.arange(2 * tile, dtype=jnp.int32)) % (2 * tile)
    bucket_hot = (bucket_of(distances)[:, None] == jnp.arange(bucket_count)).astype(f32)
    rev = jnp.sum(bias_table.astype(f32)[:, None, :] * bucket_hot[None], axis=-1)
    rev = rev.reshape(head_count // 2, 2, 2 * tile)
    key_mask = jnp.where(valid, 0.0, neg_big)[None, :].astype(f32)
    inputs_wide = inputs.astype(f32)
    scale_first = rms_scale(inputs_wide)
    normed_attn = (inputs_wide * scale_first * gain_first).astype(bf16)
    qkv = jnp.dot(normed_attn, w_proj, preferred_element_type=f32).astype(bf16)
    attn_heads, lse = attention_forward(qkv, rev, key_mask)
    hidden = inputs_wide + valid_mask * jnp.dot(attn_heads, w_mix, preferred_element_type=f32)
    scale_second = rms_scale(hidden)
    normed_moe = (hidden * scale_second * gain_second).astype(bf16)

    lanes = max(tile, 2 * expert_count)
    w_gate_wide = jnp.zeros((model_width, lanes), bf16).at[:, :expert_count].set(w_gate)
    chunks = 3
    d_normed, made, full_in, grad_w_out, router_wide = expert_pass(
        normed_moe, select.reshape(expert_count, capacity, tok_count), other, w_gate_wide, g_rows,
        w_in[0], w_out[0], chunks,
    )
    made_back = to_experts(made).reshape(rows, model_width)
    grad_w_in = lax.psum_scatter(full_in, "dp", scatter_dimension=1, tiled=True).astype(f32)[None]
    grad_w_out = grad_w_out[None]
    grad_router = router_wide[:, :expert_count] + router_wide[:, lanes // 2 : lanes // 2 + expert_count]

    moe_out = jnp.dot(select.T, made_back, preferred_element_type=f32)
    outputs = (valid_mask * (hidden + moe_out)).astype(bf16)

    d_hidden_norm, grad_gain_moe = rms_back(hidden, scale_second, gain_second, d_normed)
    d_hidden = cotangent.astype(f32) * valid_mask + d_hidden_norm
    d_proj = (d_hidden * valid_mask).astype(bf16)
    grad_attn_out = jnp.dot(attn_heads.T, d_proj, preferred_element_type=f32)
    d_heads = jnp.dot(d_proj, w_mix.T, preferred_element_type=f32).astype(bf16)
    dq, dk, dv, d_line = attention_backward(qkv, d_heads, lse, rev, key_mask)
    d_qkv = jnp.concatenate([dq, dk, dv], axis=1)
    near = jnp.arange(2 * tile, dtype=jnp.int32)
    line_hot = (bucket_of((2 * tile - near) % (2 * tile))[:, None] == jnp.arange(bucket_count)).astype(f32)
    grad_rel_bias = jnp.sum(d_line.reshape(head_count, 2 * tile, 1) * line_hot[None], axis=1)
    grad_qkv = jnp.dot(normed_attn.T, d_qkv, preferred_element_type=f32)
    d_normed_attn = jnp.dot(d_qkv, w_proj.T, preferred_element_type=f32)
    d_norm_in, grad_gain_attn = rms_back(inputs_wide, scale_first, gain_first, d_normed_attn)
    d_inputs = (d_hidden + d_norm_in).astype(bf16)

    bias_col = jnp.pad(
        grad_rel_bias.reshape(dp_count, bias_cells), ((0, 0), (0, shard - bias_cells))
    ).reshape(model_width, 1)
    small_grad = jnp.concatenate(
        [grad_router, grad_gain_attn[:, None], grad_gain_moe[:, None], bias_col], axis=1
    )
    small_grad = jnp.pad(small_grad, ((0, 0), (0, tile - small_grad.shape[1])))
    packed = jnp.concatenate([grad_qkv, grad_attn_out, small_grad], axis=1).astype(bf16)
    part = lax.psum_scatter(packed, "dp", scatter_dimension=0, tiled=True)
    whole = lax.psum(part, "expert").astype(f32)
    end = 4 * model_width
    tail = whole[:, end:]
    return (
        outputs,
        d_inputs,
        whole[:, : 3 * model_width],
        whole[:, 3 * model_width : end],
        tail[:, :expert_count],
        tail[:, expert_count],
        tail[:, expert_count + 1],
        tail[:bias_cells, expert_count + 2].reshape(rel_bias.shape),
        grad_w_in,
        grad_w_out,
    )


def solution(mesh):
    placed = (
        P(("dp", "expert"), None),
        P(("dp", "expert"), None),
        P(("dp", "expert")),
        P(("dp", "expert"), None),
        P("dp", None),
        P("dp", None),
        P("dp", None),
        P("dp"),
        P("dp"),
        P("dp", None),
        P("expert", None, None),
        P("expert", None, None),
    )
    return jax.shard_map(
        on_device,
        mesh=mesh,
        in_specs=placed,
        out_specs=(
            P(("dp", "expert"), None),
            P(("dp", "expert"), None),
            P("dp", None),
            P("dp", None),
            P("dp", None),
            P("dp"),
            P("dp"),
            P("dp", None),
            P("expert", None, "dp"),
            P("expert", None, "dp"),
        ),
        check_vma=False,
    )
```
